32 devices in a mesh: gx: 8 (over y, x, core), gy: 4 (over z).
Axes of the slice: x: 2, y: 2, z: 4, core: 2. Of those that a mesh axis runs over, the one named last changes fastest.
Arguments:
- estimate: float32 [128, 64, 128], P('gx', 'gy'), may hold values from 0.5 to 12
- recorded: float32 [2, 128, 64, 128], P(None, 'gx', 'gy'), may hold values from 0.1 to 3
- spread: float32 [2, 35937], replicated, may hold values from 2.7826474e-06 to 2.4
- background: float32 [2], replicated, may hold values from 0.2 to 1
Outputs:
- restored: float32 [128, 64, 128], P('gx', 'gy')
The draws below stay inside these ranges and needn't reach their ends.
All inputs are finite; a program needn't handle non-finite values.
Results may differ from the reference program's by a relative error of at most 0.0001.
Values sent between devices are 32-bit elements; how exact they have to be, the bound alone decides.
A program may use at most 64 MiB of HBM per device.

```python
import math
import jax
import jax.numpy as jnp

VIEWS = 2
PSF_SIZE = 33
HALO = 16
ITERS = 1
NZ = 128
NX = 128
NY = 64


def draw_recorded(key, part):
    noise_key = jax.random.fold_in(jax.random.fold_in(key, 7), 0)
    levels = 1.0 + 2.0 * jnp.arange(NX, dtype=jnp.float32) / max(NX - 1, 1)
    values = jnp.exp(jax.random.uniform(noise_key, (VIEWS, NX, NY, NZ), jnp.float32, math.log(0.2), 0.0))
    return values * levels[None, :, None, None]


def draw_estimate(key, part):
    base_key, bead_key, bright_key = jax.random.split(jax.random.fold_in(key, 11), 3)
    shape = (NX, NY, NZ)
    base = jnp.exp(jax.random.uniform(base_key, shape, jnp.float32, math.log(0.5), math.log(1.5)))
    chosen = jax.random.uniform(bead_key, shape, jnp.float32, 0.0, 1.0) < 0.04
    bright = jax.random.uniform(bright_key, shape, jnp.float32, 3.0, 8.0)
    return base * jnp.where(chosen, bright, 1.0)


def draw_spread(key, part):
    keys = jax.random.split(jax.random.fold_in(key, 23), 6)
    offsets = jnp.arange(PSF_SIZE, dtype=jnp.float32) - HALO
    along_x = offsets[None, :, None, None]
    along_y = offsets[None, None, :, None]
    along_z = offsets[None, None, None, :]
    polar = jax.random.uniform(keys[0], (VIEWS, 1, 1, 1), jnp.float32, 0.5, 1.1)
    azimuth = jax.random.uniform(keys[1], (VIEWS, 1, 1, 1), jnp.float32, 0.0, 2.0 * math.pi)
    long_sigma = 1.0 + HALO * jax.random.uniform(keys[2], (VIEWS, 1, 1, 1), jnp.float32, 0.15, 0.3)
    cross_sigma = 0.6 + HALO * jax.random.uniform(keys[3], (VIEWS, 1, 1, 1), jnp.float32, 0.04, 0.08)
    unit_x = jnp.sin(polar) * jnp.cos(azimuth)
    unit_y = jnp.sin(polar) * jnp.sin(azimuth)
    unit_z = jnp.cos(polar)
    along = unit_x * along_x + unit_y * along_y + unit_z * along_z
    square = along_x * along_x + along_y * along_y + along_z * along_z
    across = jnp.maximum(square - along * along, 0.0)
    shape = (VIEWS, PSF_SIZE, PSF_SIZE, PSF_SIZE)
    rough = jax.random.uniform(keys[4], shape, jnp.float32, 0.7, 1.3)
    core = jnp.exp(-along * along / (2.0 * long_sigma ** 2) - across / (2.0 * cross_sigma ** 2)) * rough
    total = jnp.sum(core, axis=(1, 2, 3), keepdims=True)
    floor = jax.random.uniform(keys[5], shape, jnp.float32, 0.2, 1.0) * 0.8 * total / PSF_SIZE ** 3
    return (core + floor).reshape(VIEWS, PSF_SIZE * PSF_SIZE * PSF_SIZE)


def setup_inputs(seed: int = 0) -> dict:
    seeds = jax.random.split(jax.random.key(seed), 5)
    estimate = draw_estimate(jax.random.fold_in(seeds[4], 71), 0)
    recorded = draw_recorded(jax.random.fold_in(seeds[4], 71), 0)
    spread = draw_spread(jax.random.fold_in(seeds[4], 71), 0)
    background = jnp.clip(jnp.exp(jax.random.uniform(seeds[3], (VIEWS,), jnp.float32, math.log(0.2), math.log(1.0))), 0.2, 1.0)
    return dict(estimate=estimate, recorded=recorded, spread=spread, background=background)


clip_fraction = 0.6


def kernel_spectra(spread, lengths):
    cube = spread.reshape(VIEWS, PSF_SIZE, PSF_SIZE, PSF_SIZE)
    normed = cube / jnp.sum(cube, axis=(1, 2, 3), keepdims=True)
    placed = jnp.zeros((VIEWS,) + lengths, spread.dtype)
    placed = placed.at[:, :PSF_SIZE, :PSF_SIZE, :PSF_SIZE].set(normed)
    placed = jnp.roll(placed, (-HALO, -HALO, -HALO), axis=(1, 2, 3))
    return jnp.fft.rfftn(placed, axes=(1, 2, 3))


def apply_kernel(volume, spectrum, mirrored, lengths):
    padded = jnp.pad(volume, ((0, HALO), (0, HALO), (0, HALO)))
    transformed = jnp.fft.rfftn(padded)
    factor = jnp.conj(spectrum) if mirrored else spectrum
    whole = jnp.fft.irfftn(transformed * factor, s=lengths)
    return whole[:NX, :NY, :NZ]


def reference(estimate, recorded, spread, background):
    lengths = (NX + HALO, NY + HALO, NZ + HALO)
    spectra = kernel_spectra(spread, lengths)
    current = estimate
    for iteration in range(ITERS):
        quotients = []
        for view_index in range(VIEWS):
            blurred = background[view_index] + apply_kernel(current, spectra[view_index], False, lengths)
            quotients.append(recorded[view_index] / blurred)
        stacked = jnp.stack(quotients)
        peak = jnp.max(stacked)
        clipped = jnp.minimum(stacked, clip_fraction * peak)
        summed = apply_kernel(clipped[0], spectra[0], True, lengths)
        for view_index in range(1, VIEWS):
            summed = summed + apply_kernel(clipped[view_index], spectra[view_index], True, lengths)
        current = current * (summed / VIEWS)
    return current
```

```python
import functools
import math

import jax
import jax.numpy as jnp
import numpy as np
from jax import lax
from jax.experimental import pallas as pl
from jax.experimental.pallas import tpu as pltpu
from jax.sharding import PartitionSpec as P

clip_fraction = 0.6
F32 = jnp.float32
BF16 = jnp.bfloat16
LANES = 128


def round_edge(total):
    edge = 1
    while (edge + 1) ** 3 <= total:
        edge = edge + 1
    return edge


def round_up(value, unit):
    return -(-value // unit) * unit


def three(table, axis):
    high = table.astype(jnp.bfloat16)
    low = (table - high.astype(np.float64)).astype(jnp.bfloat16)
    return np.concatenate([high, high, low], axis=axis)


def angle(outer, inner, modulus):
    return 2.0 * math.pi / modulus * (np.outer(outer, inner) % modulus)


def plane_table(outputs, inputs, modulus, factor, width):
    theta = angle(outputs, inputs, modulus)
    table = np.zeros((2 * len(outputs), width))
    table[: len(outputs), : len(inputs)] = factor * np.cos(theta)
    table[len(outputs) :, : len(inputs)] = factor * np.sin(theta)
    return three(table, 1)


def depth_table(positions, count, modulus, rows, half):
    theta = angle(positions, np.arange(count), modulus)
    table = np.zeros((rows, 2 * half))
    table[: len(positions), :count] = np.cos(theta)
    table[: len(positions), half : half + count] = -np.sin(theta)
    return three(table, 0)


def depth_inverse(count, length, modulus, half):
    freqs = np.arange(count)
    theta = angle(freqs, np.arange(length), modulus)
    weight = np.where((freqs == 0) | (2 * freqs == modulus), 1.0, 2.0) / modulus
    table = np.zeros((2 * half, length))
    table[:count] = weight[:, None] * np.cos(theta)
    table[half : half + count] = -weight[:, None] * np.sin(theta)
    return three(table, 0)


def axis_tables(cells, reach, size):
    width = cells + 2 * reach
    whole = np.arange(width)
    own = reach + np.arange(cells)
    return [
        plane_table(whole, whole, width, 1.0, width),
        plane_table(whole, np.arange(size) - reach, width, 1.0, width),
        plane_table(whole, own, width, 1.0, cells),
        plane_table(own, whole, width, 1.0 / width, width),
        plane_table(whole, whole, width, 1.0 / width, width),
    ]


def split3(x, axis):
    high = x.astype(BF16)
    low = (x - high.astype(F32)).astype(BF16)
    return jnp.concatenate([high, low, high], axis=axis)


def along_depth(x, table):
    return jnp.dot(split3(x, 1), table, preferred_element_type=F32)


def along_plane(x, table, inverse):
    both = jnp.dot(table, split3(x, 0), preferred_element_type=F32)
    count, half = both.shape[0] // 2, both.shape[1] // 2
    direct, crossed = both[:count], both[count:]
    real, imag = crossed[:, :half], crossed[:, half:]
    if inverse:
        return direct[:, :half] - imag, direct[:, half:] + real
    return direct[:, :half] + imag, direct[:, half:] - real


def body(
    nx, ny, reach, size,
    est, rec, cube, back, tz, tzk, tzi,
    xf, xk, xo, xc, xw, yf, yk, yo, yc, yw,
    out,
    win, spec, work, s3, quot, s2b, ow, rx, ry, pkx, pky,
    send, recv, sendx, recvx, sendy, recvy,
):
    views = rec.shape[0]
    cx, cy, depth = est.shape
    wx, wy = cx + 2 * reach, cy + 2 * reach
    half = tz.shape[1] // 2
    gx, gy = lax.axis_index("gx"), lax.axis_index("gy")
    right, left = {"gx": lax.rem(gx + 1, nx)}, {"gx": lax.rem(gx + nx - 1, nx)}
    above, below = {"gy": lax.rem(gy + 1, ny)}, {"gy": lax.rem(gy + ny - 1, ny)}
    has = {"right": gx < nx - 1, "left": gx > 0, "above": gy < ny - 1, "below": gy > 0}

    barrier = pltpu.get_barrier_semaphore()
    for d in range(1, nx):
        pl.semaphore_signal(
            barrier, inc=1, device_id={"gx": lax.rem(gx + d, nx)}, device_id_type=pl.DeviceIdType.MESH
        )
    for d in range(1, ny):
        pl.semaphore_signal(
            barrier, inc=1, device_id={"gy": lax.rem(gy + d, ny)}, device_id_type=pl.DeviceIdType.MESH
        )
    pl.semaphore_wait(barrier, nx + ny - 2)

    def copy(src, dst, k, target):
        return pltpu.make_async_remote_copy(
            src_ref=src, dst_ref=dst, send_sem=send.at[k], recv_sem=recv.at[k],
            device_id=target, device_id_type=pl.DeviceIdType.MESH,
        )

    def start(c, to):
        @pl.when(has[to])
        def _():
            c.start()

    def wait_send(c, to):
        @pl.when(has[to])
        def _():
            c.wait_send()

    def wait_recv(c, source):
        @pl.when(has[source])
        def _():
            c.wait_recv()

    hx, hy = pl.ds(reach, cx), pl.ds(reach, cy)
    low, high_x, high_y = pl.ds(0, reach), pl.ds(reach + cx, reach), pl.ds(reach + cy, reach)
    last_x, first = pl.ds(cx, reach), pl.ds(reach, reach)
    y_up = copy(est.at[:, pl.ds(cy - reach, reach)], win.at[hx, low], 0, above)
    y_down = copy(est.at[:, low], win.at[hx, high_y], 1, below)
    x_up = [copy(est.at[pl.ds(cx - reach, reach)], win.at[low, hy], 2, right)]
    x_down = [copy(est.at[low], win.at[high_x, hy], 3, left)]
    for n, strip in enumerate((low, high_y)):
        x_up.append(copy(win.at[last_x, strip], win.at[low, strip], 4 + 2 * n, right))
        x_down.append(copy(win.at[first, strip], win.at[high_x, strip], 5 + 2 * n, left))
    start(y_up, "above")
    start(y_down, "below")
    start(x_up[0], "right")
    start(x_down[0], "left")

    win[hx, hy] = est[...]

    @pl.when(gy == 0)
    def _():
        win[hx, low] = jnp.zeros((cx, reach, depth), F32)

    @pl.when(gy == ny - 1)
    def _():
        win[hx, high_y] = jnp.zeros((cx, reach, depth), F32)

    @pl.when(gx == 0)
    def _():
        win[low] = jnp.zeros((reach, wy, depth), F32)

    @pl.when(gx == nx - 1)
    def _():
        win[high_x] = jnp.zeros((reach, wy, depth), F32)

    def put(ref, index, rows, pair):
        ref[index + (0, rows)] = pair[0]
        ref[index + (1, rows)] = pair[1]

    def get(ref, index, rows):
        return jnp.concatenate([ref[index + (0, rows)], ref[index + (1, rows)]], axis=1)

    step = math.gcd(wx, 8)

    def depth_then_y(load, count, table, plane):
        def go(c, carry):
            spectrum = along_depth(load(c), table)
            for n in range(step):
                pair = along_plane(spectrum[n * wy : (n + 1) * wy], plane, False)
                put(work, (), pl.ds(pl.multiple_of((c * step + n) * wy, 8), wy), pair)
            return carry

        lax.fori_loop(0, count, go, 0)

    def kernel_spectrum(v):
        blocks = -(-size // step)
        scale = 1.0 / jnp.sum(cube[v])
        depth_then_y(
            lambda c: cube[v, pl.ds(pl.multiple_of(c * step * wy, 8), step * wy)], blocks, tzk[...], yk[...]
        )
        rest = wx * wy - blocks * step * wy
        if rest:
            for h in range(2):
                work[h, pl.ds(blocks * step * wy, rest)] = jnp.zeros((rest, half), F32)

        def go(q, carry):
            pair = along_plane(get(work, (), pl.ds(q, wx, stride=wy)), xk[...], False)
            pair = (pair[0] * scale, pair[1] * scale)
            put(spec, (v,), pl.ds(pl.multiple_of(q * wx, 8), wx), pair)
            return carry

        lax.fori_loop(0, wy, go, 0, unroll=4)

    kernel_spectrum(0)

    wait_recv(y_up, "below")
    wait_recv(y_down, "above")
    for c in x_up[1:]:
        start(c, "right")
    for c in x_down[1:]:
        start(c, "left")

    for v in range(1, views):
        kernel_spectrum(v)

    for c in x_up:
        wait_recv(c, "left")
    for c in x_down:
        wait_recv(c, "right")

    depth_then_y(
        lambda c: win[pl.ds(c * step, step)].reshape(step * wy, depth), wx // step, tz[...], yf[...]
    )

    def filter_forward(q, carry):
        real, imag = along_plane(get(work, (), pl.ds(q, wx, stride=wy)), xf[...], False)
        rows = pl.ds(pl.multiple_of(q * wx, 8), wx)
        for v in range(views):
            kr, ki = spec[v, 0, rows], spec[v, 1, rows]
            product = jnp.concatenate([real * kr - imag * ki, real * ki + imag * kr], axis=1)
            put(s3, (v,), pl.ds(pl.multiple_of(q * cx, 8), cx), along_plane(product, xc[...], True))
        return carry

    lax.fori_loop(0, wy, filter_forward, 0, unroll=4)

    tops = jnp.zeros((8, depth), F32)
    for v in range(views):
        planes = []
        for x in range(cx):
            pair = along_plane(get(s3, (v,), pl.ds(x, wy, stride=cx)), yc[...], True)
            planes.append(jnp.concatenate(pair, axis=1))
        blurred = along_depth(jnp.concatenate(planes, axis=0), tzi[...]) + back[v]
        quotient = rec[v].reshape(cx * cy, depth) / blurred
        quot[v] = quotient
        top = jnp.max(quotient.reshape(cx * cy // 8, 8, depth), axis=0)
        tops = top if v == 0 else jnp.maximum(tops, top)

    def spread_peak(axis, me, count, slots, send_sems, recv_sems):
        copies = []
        for d in range(1, count):
            copies.append(
                pltpu.make_async_remote_copy(
                    src_ref=slots.at[0], dst_ref=slots.at[d], send_sem=send_sems.at[d],
                    recv_sem=recv_sems.at[d], device_id={axis: lax.rem(me + d, count)},
                    device_id_type=pl.DeviceIdType.MESH,
                )
            )
        for c in copies:
            c.start()
        for c in copies:
            c.wait()

    pkx[0] = tops
    spread_peak("gx", gx, nx, pkx, sendx, recvx)
    pky[0] = jnp.max(pkx[...], axis=0)
    spread_peak("gy", gy, ny, pky, sendy, recvy)
    limit = clip_fraction * jnp.max(jnp.max(pky[...], axis=0))

    for v in range(views):
        spectrum = along_depth(jnp.minimum(quot[v], limit), tz[...])
        for x in range(cx):
            pair = along_plane(spectrum[x * cy : (x + 1) * cy], yo[...], False)
            put(s2b, (v,), pl.ds(x * wy, wy), pair)

    def filter_back(q, carry):
        rows = pl.ds(pl.multiple_of(q * wx, 8), wx)
        real = imag = None
        for v in range(views):
            ar, ai = along_plane(get(s2b, (v,), pl.ds(q, cx, stride=wy)), xo[...], False)
            kr, ki = spec[v, 0, rows], spec[v, 1, rows]
            pr, pi = ar * kr + ai * ki, ai * kr - ar * ki
            real, imag = (pr, pi) if v == 0 else (real + pr, imag + pi)
        put(work, (), rows, along_plane(jnp.concatenate([real, imag], axis=1), xw[...], True))
        return carry

    lax.fori_loop(0, wy, filter_back, 0, unroll=4)

    few = math.gcd(math.gcd(reach, cx), 8)

    def finish_slab(begin, count):
        def go(c, carry):
            planes = []
            for n in range(few):
                pair = along_plane(get(work, (), pl.ds(begin + c * few + n, wy, stride=wx)), yw[...], True)
                planes.append(jnp.concatenate(pair, axis=1))
            volume = along_depth(jnp.concatenate(planes, axis=0), tzi[...])
            ow[pl.ds(begin + c * few, few)] = volume.reshape(few, wy, depth)
            return carry

        lax.fori_loop(0, count // few, go, 0)

    to_left = copy(ow.at[low], rx.at[0], 8, left)
    to_right = copy(ow.at[high_x], rx.at[1], 9, right)
    to_below = copy(ow.at[hx, low], ry.at[0], 10, below)
    to_above = copy(ow.at[hx, high_y], ry.at[1], 11, above)
    finish_slab(0, reach)
    start(to_left, "left")
    finish_slab(reach + cx, reach)
    start(to_right, "right")
    finish_slab(reach, cx)

    @pl.when(has["right"])
    def _():
        to_left.wait_recv()
        ow[last_x] = ow[last_x] + rx[0]

    @pl.when(has["left"])
    def _():
        to_right.wait_recv()
        ow[first] = ow[first] + rx[1]

    start(to_below, "below")
    start(to_above, "above")

    @pl.when(has["above"])
    def _():
        to_below.wait_recv()
        ow[hx, pl.ds(cy, reach)] = ow[hx, pl.ds(cy, reach)] + ry[0]

    @pl.when(has["below"])
    def _():
        to_above.wait_recv()
        ow[hx, first] = ow[hx, first] + ry[1]

    out[...] = est[...] * (ow[hx, hy] / views)

    wait_send(y_up, "above")
    wait_send(y_down, "below")
    for c in x_up + [to_right]:
        wait_send(c, "right")
    for c in x_down + [to_left]:
        wait_send(c, "left")
    wait_send(to_below, "below")
    wait_send(to_above, "above")


def on_device(nx, ny, estimate, recorded, spread, background):
    views = spread.shape[0]
    size = round_edge(spread.shape[1])
    reach = size // 2
    cx, cy, depth = estimate.shape
    wx, wy = cx + 2 * reach, cy + 2 * reach
    period = depth + reach
    freqs = period // 2 + 1
    half = round_up(freqs, LANES)
    taps = round_up(size, LANES)
    cube = jnp.pad(
        spread.reshape(views, size, size, size),
        ((0, 0), (0, wx - size), (0, wy - size), (0, taps - size)),
    ).reshape(views, wx * wy, taps)
    tables = [
        depth_table(np.arange(depth), freqs, period, depth, half),
        depth_table(np.arange(size) - reach, freqs, period, taps, half),
        depth_inverse(freqs, depth, period, half),
    ]
    tables += axis_tables(cx, reach, size) + axis_tables(cy, reach, size)
    vmem = pl.BlockSpec(memory_space=pltpu.VMEM)
    smem = pl.BlockSpec(memory_space=pltpu.SMEM)
    dma = pltpu.SemaphoreType.DMA
    return pl.pallas_call(
        functools.partial(body, nx, ny, reach, size),
        out_shape=jax.ShapeDtypeStruct(estimate.shape, estimate.dtype),
        in_specs=[vmem, vmem, vmem, smem] + [vmem] * len(tables),
        out_specs=vmem,
        scratch_shapes=[
            pltpu.VMEM((wx, wy, depth), F32),
            pltpu.VMEM((views, 2, wx * wy, half), F32),
            pltpu.VMEM((2, wx * wy, half), F32),
            pltpu.VMEM((views, 2, cx * wy, half), F32),
            pltpu.VMEM((views, cx * cy, depth), F32),
            pltpu.VMEM((views, 2, cx * wy, half), F32),
            pltpu.VMEM((wx, wy, depth), F32),
            pltpu.VMEM((2, reach, wy, depth), F32),
            pltpu.VMEM((2, cx, reach, depth), F32),
            pltpu.VMEM((nx, 8, depth), F32),
            pltpu.VMEM((ny, 8, depth), F32),
            dma((12,)), dma((12,)),
            dma((nx,)), dma((nx,)),
            dma((ny,)), dma((ny,)),
        ],
        compiler_params=pltpu.CompilerParams(
            collective_id=0, has_side_effects=True, vmem_limit_bytes=60 * 1024 * 1024
        ),
    )(estimate, recorded, cube, background, *[jnp.asarray(t) for t in tables])


def solution(mesh):
    in_specs = (P("gx", "gy", None), P(None, "gx", "gy", None), P(), P())
    return jax.shard_map(
        functools.partial(on_device, mesh.shape["gx"], mesh.shape["gy"]),
        mesh=mesh, in_specs=in_specs, out_specs=P("gx", "gy", None), check_vma=False,
    )
```

```python
import functools
import math

import jax
import jax.numpy as jnp
import numpy as np
from jax import lax
from jax.experimental import pallas as pl
from jax.experimental.pallas import tpu as pltpu
from jax.sharding import PartitionSpec as P

clip_fraction = 0.6
F32 = jnp.float32
BF16 = jnp.bfloat16
LANES = 128


def round_edge(total):
    edge = 1
    while (edge + 1) ** 3 <= total:
        edge = edge + 1
    return edge


def round_up(value, unit):
    return -(-value // unit) * unit


def three(table, axis):
    high = table.astype(jnp.bfloat16)
    low = (table - high.astype(np.float64)).astype(jnp.bfloat16)
    return np.concatenate([high, high, low], axis=axis)


def angle(outer, inner, modulus):
    return 2.0 * math.pi / modulus * (np.outer(outer, inner) % modulus)


def plane_table(outputs, inputs, modulus, factor, width):
    theta = angle(outputs, inputs, modulus)
    table = np.zeros((2 * len(outputs), width))
    table[: len(outputs), : len(inputs)] = factor * np.cos(theta)
    table[len(outputs) :, : len(inputs)] = factor * np.sin(theta)
    return three(table, 1)


def depth_table(positions, count, modulus, rows, half):
    theta = angle(positions, np.arange(count), modulus)
    table = np.zeros((rows, 2 * half))
    table[: len(positions), :count] = np.cos(theta)
    table[: len(positions), half : half + count] = -np.sin(theta)
    return three(table, 0)


def depth_inverse(count, length, modulus, half):
    freqs = np.arange(count)
    theta = angle(freqs, np.arange(length), modulus)
    weight = np.where((freqs == 0) | (2 * freqs == modulus), 1.0, 2.0) / modulus
    table = np.zeros((2 * half, length))
    table[:count] = weight[:, None] * np.cos(theta)
    table[half : half + count] = -weight[:, None] * np.sin(theta)
    return three(table, 0)


def axis_tables(cells, reach, size):
    width = cells + 2 * reach
    whole = np.arange(width)
    own = reach + np.arange(cells)
    return [
        plane_table(whole, whole, width, 1.0, width),
        plane_table(whole, np.arange(size) - reach, width, 1.0, width),
        plane_table(whole, own, width, 1.0, cells),
        plane_table(own, whole, width, 1.0 / width, width),
        plane_table(whole, whole, width, 1.0 / width, width),
    ]


def split3(x, axis):
    high = x.astype(BF16)
    low = (x - high.astype(F32)).astype(BF16)
    return jnp.concatenate([high, low, high], axis=axis)


def along_depth(x, table):
    return jnp.dot(split3(x, 1), table, preferred_element_type=F32)


def along_plane(x, table, inverse):
    both = jnp.dot(table, split3(x, 0), preferred_element_type=F32)
    count, half = both.shape[0] // 2, both.shape[1] // 2
    direct, crossed = both[:count], both[count:]
    real, imag = crossed[:, :half], crossed[:, half:]
    if inverse:
        return direct[:, :half] - imag, direct[:, half:] + real
    return direct[:, :half] + imag, direct[:, half:] - real


def body(
    nx, ny, reach, size,
    est, rec, cube, back, tz, tzk, tzi,
    xf, xk, xo, xc, xw, yf, yk, yo, yc, yw,
    out,
    win, spec, work, s3, quot, s2b, ow, rx, ry, pkx, pky,
    send, recv, sendx, recvx, sendy, recvy,
):
    views = rec.shape[0]
    cx, cy, depth = est.shape
    wx, wy = cx + 2 * reach, cy + 2 * reach
    half = tz.shape[1] // 2
    px, py, pc = wx + 1, wy + 1, cx + 1
    gx, gy = lax.axis_index("gx"), lax.axis_index("gy")
    right, left = {"gx": lax.rem(gx + 1, nx)}, {"gx": lax.rem(gx + nx - 1, nx)}
    above, below = {"gy": lax.rem(gy + 1, ny)}, {"gy": lax.rem(gy + ny - 1, ny)}
    has = {"right": gx < nx - 1, "left": gx > 0, "above": gy < ny - 1, "below": gy > 0}

    barrier = pltpu.get_barrier_semaphore()
    for d in range(1, nx):
        pl.semaphore_signal(
            barrier, inc=1, device_id={"gx": lax.rem(gx + d, nx)}, device_id_type=pl.DeviceIdType.MESH
        )
    for d in range(1, ny):
        pl.semaphore_signal(
            barrier, inc=1, device_id={"gy": lax.rem(gy + d, ny)}, device_id_type=pl.DeviceIdType.MESH
        )
    pl.semaphore_wait(barrier, nx + ny - 2)

    def copy(src, dst, k, target):
        return pltpu.make_async_remote_copy(
            src_ref=src, dst_ref=dst, send_sem=send.at[k], recv_sem=recv.at[k],
            device_id=target, device_id_type=pl.DeviceIdType.MESH,
        )

    def start(c, to):
        @pl.when(has[to])
        def _():
            c.start()

    def wait_send(c, to):
        @pl.when(has[to])
        def _():
            c.wait_send()

    def wait_recv(c, source):
        @pl.when(has[source])
        def _():
            c.wait_recv()

    hx, hy = pl.ds(reach, cx), pl.ds(reach, cy)
    low, high_x, high_y = pl.ds(0, reach), pl.ds(reach + cx, reach), pl.ds(reach + cy, reach)
    last_x, first = pl.ds(cx, reach), pl.ds(reach, reach)
    y_up = copy(est.at[:, pl.ds(cy - reach, reach)], win.at[hx, low], 0, above)
    y_down = copy(est.at[:, low], win.at[hx, high_y], 1, below)
    x_up = [copy(est.at[pl.ds(cx - reach, reach)], win.at[low, hy], 2, right)]
    x_down = [copy(est.at[low], win.at[high_x, hy], 3, left)]
    for n, strip in enumerate((low, high_y)):
        x_up.append(copy(win.at[last_x, strip], win.at[low, strip], 4 + 2 * n, right))
        x_down.append(copy(win.at[first, strip], win.at[high_x, strip], 5 + 2 * n, left))
    start(y_up, "above")
    start(y_down, "below")
    start(x_up[0], "right")
    start(x_down[0], "left")

    win[hx, hy] = est[...]

    @pl.when(gy == 0)
    def _():
        win[hx, low] = jnp.zeros((cx, reach, depth), F32)

    @pl.when(gy == ny - 1)
    def _():
        win[hx, high_y] = jnp.zeros((cx, reach, depth), F32)

    @pl.when(gx == 0)
    def _():
        win[low] = jnp.zeros((reach, wy, depth), F32)

    @pl.when(gx == nx - 1)
    def _():
        win[high_x] = jnp.zeros((reach, wy, depth), F32)

    def put(ref, index, rows, pair):
        ref[index + (0, rows)] = pair[0]
        ref[index + (1, rows)] = pair[1]

    def get(ref, index, rows):
        return jnp.concatenate([ref[index + (0, rows)], ref[index + (1, rows)]], axis=1)

    step = math.gcd(wx, 8)

    def depth_then_y(load, count, table, plane):
        def go(c, carry):
            spectrum = along_depth(load(c), table)
            for n in range(step):
                pair = along_plane(spectrum[n * wy : (n + 1) * wy], plane, False)
                put(work, (), pl.ds((c * step + n) * py, wy), pair)
            return carry

        lax.fori_loop(0, count, go, 0)

    def kernel_spectrum(v):
        blocks = -(-size // step)
        scale = 1.0 / jnp.sum(cube[v])
        depth_then_y(
            lambda c: cube[v, pl.ds(pl.multiple_of(c * step * wy, 8), step * wy)], blocks, tzk[...], yk[...]
        )
        rest = (wx - blocks * step) * py
        if rest:
            for h in range(2):
                work[h, pl.ds(blocks * step * py, rest)] = jnp.zeros((rest, half), F32)

        def go(q, carry):
            pair = along_plane(get(work, (), pl.ds(q, wx, stride=py)), xk[...], False)
            pair = (pair[0] * scale, pair[1] * scale)
            put(spec, (v,), pl.ds(pl.multiple_of(q * wx, 8), wx), pair)
            return carry

        lax.fori_loop(0, wy, go, 0, unroll=4)

    kernel_spectrum(0)

    wait_recv(y_up, "below")
    wait_recv(y_down, "above")
    for c in x_up[1:]:
        start(c, "right")
    for c in x_down[1:]:
        start(c, "left")

    for v in range(1, views):
        kernel_spectrum(v)

    for c in x_up:
        wait_recv(c, "left")
    for c in x_down:
        wait_recv(c, "right")

    depth_then_y(
        lambda c: win[pl.ds(c * step, step)].reshape(step * wy, depth), wx // step, tz[...], yf[...]
    )

    def filter_forward(q, carry):
        real, imag = along_plane(get(work, (), pl.ds(q, wx, stride=py)), xf[...], False)
        rows = pl.ds(pl.multiple_of(q * wx, 8), wx)
        for v in range(views):
            kr, ki = spec[v, 0, rows], spec[v, 1, rows]
            product = jnp.concatenate([real * kr - imag * ki, real * ki + imag * kr], axis=1)
            put(s3, (v,), pl.ds(q * pc, cx), along_plane(product, xc[...], True))
        return carry

    lax.fori_loop(0, wy, filter_forward, 0, unroll=4)

    tops = jnp.zeros((8, depth), F32)
    for v in range(views):
        planes = []
        for x in range(cx):
            pair = along_plane(get(s3, (v,), pl.ds(x, wy, stride=pc)), yc[...], True)
            planes.append(jnp.concatenate(pair, axis=1))
        blurred = along_depth(jnp.concatenate(planes, axis=0), tzi[...]) + back[v]
        quotient = rec[v].reshape(cx * cy, depth) / blurred
        quot[v] = quotient
        top = jnp.max(quotient.reshape(cx * cy // 8, 8, depth), axis=0)
        tops = top if v == 0 else jnp.maximum(tops, top)

    def spread_peak(axis, me, count, slots, send_sems, recv_sems):
        copies = []
        for d in range(1, count):
            copies.append(
                pltpu.make_async_remote_copy(
                    src_ref=slots.at[0], dst_ref=slots.at[d], send_sem=send_sems.at[d],
                    recv_sem=recv_sems.at[d], device_id={axis: lax.rem(me + d, count)},
                    device_id_type=pl.DeviceIdType.MESH,
                )
            )
        for c in copies:
            c.start()
        for c in copies:
            c.wait()

    pkx[0] = tops
    spread_peak("gx", gx, nx, pkx, sendx, recvx)
    pky[0] = jnp.max(pkx[...], axis=0)
    spread_peak("gy", gy, ny, pky, sendy, recvy)
    limit = clip_fraction * jnp.max(jnp.max(pky[...], axis=0))

    for v in range(views):
        spectrum = along_depth(jnp.minimum(quot[v], limit), tz[...])
        for x in range(cx):
            pair = along_plane(spectrum[x * cy : (x + 1) * cy], yo[...], False)
            put(s2b, (v,), pl.ds(x * py, wy), pair)

    def filter_back(q, carry):
        rows = pl.ds(pl.multiple_of(q * wx, 8), wx)
        real = imag = None
        for v in range(views):
            ar, ai = along_plane(get(s2b, (v,), pl.ds(q, cx, stride=py)), xo[...], False)
            kr, ki = spec[v, 0, rows], spec[v, 1, rows]
            pr, pi = ar * kr + ai * ki, ai * kr - ar * ki
            real, imag = (pr, pi) if v == 0 else (real + pr, imag + pi)
        put(work, (), pl.ds(q * px, wx), along_plane(jnp.concatenate([real, imag], axis=1), xw[...], True))
        return carry

    lax.fori_loop(0, wy, filter_back, 0, unroll=4)

    few = math.gcd(math.gcd(reach, cx), 8)

    def finish_slab(begin, count):
        def go(c, carry):
            planes = []
            for n in range(few):
                pair = along_plane(get(work, (), pl.ds(begin + c * few + n, wy, stride=px)), yw[...], True)
                planes.append(jnp.concatenate(pair, axis=1))
            volume = along_depth(jnp.concatenate(planes, axis=0), tzi[...])
            ow[pl.ds(begin + c * few, few)] = volume.reshape(few, wy, depth)
            return carry

        lax.fori_loop(0, count // few, go, 0)

    strips = (low, high_y, hy)
    to_left = [copy(ow.at[low, t], rx.at[0, :, t], 8 + n, left) for n, t in enumerate(strips)]
    to_right = [copy(ow.at[high_x, t], rx.at[1, :, t], 13 + n, right) for n, t in enumerate(strips)]
    to_below = copy(ow.at[hx, low], ry.at[0], 11, below)
    to_above = copy(ow.at[hx, high_y], ry.at[1], 12, above)
    finish_slab(0, reach)
    for c in to_left:
        start(c, "left")
    finish_slab(reach + cx, reach)
    for c in to_right:
        start(c, "right")
    finish_slab(reach, cx)

    def add_slabs(n):
        @pl.when(has["right"])
        def _():
            to_left[n].wait_recv()
            ow[last_x, strips[n]] = ow[last_x, strips[n]] + rx[0, :, strips[n]]

        @pl.when(has["left"])
        def _():
            to_right[n].wait_recv()
            ow[first, strips[n]] = ow[first, strips[n]] + rx[1, :, strips[n]]

    add_slabs(0)
    start(to_below, "below")
    add_slabs(1)
    start(to_above, "above")
    add_slabs(2)

    @pl.when(has["above"])
    def _():
        to_below.wait_recv()
        ow[hx, pl.ds(cy, reach)] = ow[hx, pl.ds(cy, reach)] + ry[0]

    @pl.when(has["below"])
    def _():
        to_above.wait_recv()
        ow[hx, first] = ow[hx, first] + ry[1]

    out[...] = est[...] * (ow[hx, hy] / views)

    wait_send(y_up, "above")
    wait_send(y_down, "below")
    for c in x_up + to_right:
        wait_send(c, "right")
    for c in x_down + to_left:
        wait_send(c, "left")
    wait_send(to_below, "below")
    wait_send(to_above, "above")


def on_device(nx, ny, estimate, recorded, spread, background):
    views = spread.shape[0]
    size = round_edge(spread.shape[1])
    reach = size // 2
    cx, cy, depth = estimate.shape
    wx, wy = cx + 2 * reach, cy + 2 * reach
    period = depth + reach
    freqs = period // 2 + 1
    half = round_up(freqs, LANES)
    taps = round_up(size, LANES)
    cube = jnp.pad(
        spread.reshape(views, size, size, size),
        ((0, 0), (0, wx - size), (0, wy - size), (0, taps - size)),
    ).reshape(views, wx * wy, taps)
    tables = [
        depth_table(np.arange(depth), freqs, period, depth, half),
        depth_table(np.arange(size) - reach, freqs, period, taps, half),
        depth_inverse(freqs, depth, period, half),
    ]
    tables += axis_tables(cx, reach, size) + axis_tables(cy, reach, size)
    vmem = pl.BlockSpec(memory_space=pltpu.VMEM)
    smem = pl.BlockSpec(memory_space=pltpu.SMEM)
    dma = pltpu.SemaphoreType.DMA
    return pl.pallas_call(
        functools.partial(body, nx, ny, reach, size),
        out_shape=jax.ShapeDtypeStruct(estimate.shape, estimate.dtype),
        in_specs=[vmem, vmem, vmem, smem] + [vmem] * len(tables),
        out_specs=vmem,
        scratch_shapes=[
            pltpu.VMEM((wx, wy, depth), F32),
            pltpu.VMEM((views, 2, wx * wy, half), F32),
            pltpu.VMEM((2, max(wx * (wy + 1), wy * (wx + 1)), half), F32),
            pltpu.VMEM((views, 2, (cx + 1) * wy, half), F32),
            pltpu.VMEM((views, cx * cy, depth), F32),
            pltpu.VMEM((views, 2, cx * (wy + 1), half), F32),
            pltpu.VMEM((wx, wy, depth), F32),
            pltpu.VMEM((2, reach, wy, depth), F32),
            pltpu.VMEM((2, cx, reach, depth), F32),
            pltpu.VMEM((nx, 8, depth), F32),
            pltpu.VMEM((ny, 8, depth), F32),
            dma((16,)), dma((16,)),
            dma((nx,)), dma((nx,)),
            dma((ny,)), dma((ny,)),
        ],
        compiler_params=pltpu.CompilerParams(
            collective_id=0, has_side_effects=True, vmem_limit_bytes=60 * 1024 * 1024
        ),
    )(estimate, recorded, cube, background, *[jnp.asarray(t) for t in tables])


def solution(mesh):
    in_specs = (P("gx", "gy", None), P(None, "gx", "gy", None), P(), P())
    return jax.shard_map(
        functools.partial(on_device, mesh.shape["gx"], mesh.shape["gy"]),
        mesh=mesh, in_specs=in_specs, out_specs=P("gx", "gy", None), check_vma=False,
    )
```
